32 devices in a mesh: grp: 8 (over y, x, core), fsdp: 4 (over z).
Axes of the slice: x: 2, y: 2, z: 4, core: 2. Of those that a mesh axis runs over, the one named last changes fastest.
Arguments:
- layer_inputs: bfloat16 [8, 2048, 2048], P('grp', 'fsdp'), may hold values from -6 to 6
- key_cotangent: bfloat16 [8, 2048, 768], P('grp', 'fsdp'), may hold values from -0.099609375 to 0.099609375
- key_weights: bfloat16 [2048, 768], P('fsdp'), may hold values from -0.125 to 0.125
- outer_momentum: float32 [2048, 768], P('fsdp'), may hold values from -0.02 to 0.02
- state_codes: int32 [8, 2048, 768], P('grp', 'fsdp'), may hold values from 0 to 255
- first_row_max: float32 [8, 2048], P('grp', 'fsdp'), may hold values from 0.1 to 2
- first_col_max: float32 [8, 768], P('grp'), may hold values from 0.1 to 2
- second_row_max: float32 [8, 2048], P('grp', 'fsdp'), may hold values from 0.1 to 4
- second_col_max: float32 [8, 768], P('grp'), may hold values from 0.1 to 4
Outputs:
- new_weights: float32 [2048, 768], P('fsdp')
- new_momentum: float32 [2048, 768], P('fsdp')
- first_state: bfloat16 [8, 2048, 768], P('grp', 'fsdp')
- second_state: bfloat16 [8, 2048, 768], P('grp', 'fsdp')
- new_first_row_max: float32 [8, 2048], P('grp', 'fsdp')
- new_first_col_max: float32 [8, 768], P('grp')
- new_second_row_max: float32 [8, 2048], P('grp', 'fsdp')
- new_second_col_max: float32 [8, 768], P('grp')
- next_keys: bfloat16 [8, 2048, 768], P('grp', 'fsdp')
The draws below stay inside these ranges and needn't reach their ends.
All inputs are finite; a program needn't handle non-finite values. Where the reference program divides by a largest or mean magnitude, that divisor is 1e-20 or more.
Results may differ from the reference program's by a relative error of at most 0.018.
Values may be sent and summed in bfloat16 or wider, within the bound.
A program may use at most 64 MiB of HBM per device.

```python
import math
import jax
import jax.numpy as jnp
from jax import lax

ROWS = 2048
COLS = 768
TOK_DEV = 512
GROUPS = 8
TOK_GRP = 2048
N_GRP = 8
N_FSDP = 4


def set_ends(result, own_key, low, top_value):
    place = [jax.random.randint(jax.random.fold_in(own_key, axis), (), 0, length) for axis, length in enumerate(result.shape)]
    main_axis = result.shape.index(max(result.shape))
    beside = place[:main_axis] + [(place[main_axis] + 1) % result.shape[main_axis]] + place[main_axis + 1:]
    return result.at[tuple(place)].set(low).at[tuple(beside)].set(top_value)


def shard_levels(own_key, shape, shards, smallest, high):
    level = 1.0
    for position, shards_of in shards:
        steps = jax.random.uniform(jax.random.fold_in(jax.random.fold_in(own_key, 6), position), (shards_of,), jnp.float32, smallest / len(shards), high / len(shards))
        level = level * jnp.repeat(jnp.exp(steps), shape[position] // shards_of).reshape((-1,) + (1,) * (len(shape) - 1 - position))
    return level


def bell_draw(stream_key, shape, width, bound, cuts=(), dtype=jnp.bfloat16):
    entries = jax.random.normal(stream_key, shape, jnp.float32) * width
    if len(cuts) > 0:
        entries = shard_levels(stream_key, shape, cuts, -0.22, 0.18) * entries
    return jnp.clip(entries, min=-bound, max=bound).astype(dtype)


def setup_inputs(seed: int = 0) -> dict:
    streams_of = jax.random.split(jax.random.key(seed), 10)
    layer_inputs = bell_draw(streams_of[0], (GROUPS, TOK_GRP, ROWS), 1.0, 6.0, ((0, 8), (1, 4)))
    key_cotangent = bell_draw(streams_of[1], (GROUPS, TOK_GRP, COLS), 0.015625, 0.099609375, ((0, 8), (1, 4)))
    key_weights = bell_draw(streams_of[2], (ROWS, COLS), ROWS ** -0.5, 0.125, ((0, 4),))
    outer_momentum = bell_draw(streams_of[3], (ROWS, COLS), 0.003, 0.02, ((0, 4),), jnp.float32)
    state_codes = set_ends(jax.random.randint(streams_of[4], (GROUPS, ROWS, COLS), 0, 256), jax.random.fold_in(streams_of[4], 1), 0, 255).astype(jnp.int32)
    first_row_max = jnp.clip(jnp.exp(math.log(2.0) - 2.9957323 * jax.random.uniform(streams_of[5], (GROUPS, ROWS), jnp.float32) ** shard_levels(streams_of[5], (GROUPS, ROWS), ((0, 8), (1, 4)), -0.2, 0.2)), 0.1, 2.0)
    first_col_max = jnp.clip(jnp.exp(math.log(2.0) - 2.9957323 * jax.random.uniform(streams_of[6], (GROUPS, COLS), jnp.float32) ** shard_levels(streams_of[6], (GROUPS, COLS), ((0, 8),), -0.2, 0.2)), 0.1, 2.0)
    second_row_max = jnp.clip(jnp.exp(math.log(4.0) - 3.6888794 * jax.random.uniform(streams_of[7], (GROUPS, ROWS), jnp.float32) ** shard_levels(streams_of[7], (GROUPS, ROWS), ((0, 8), (1, 4)), -0.2, 0.2)), 0.1, 4.0)
    second_col_max = jnp.clip(jnp.exp(math.log(4.0) - 3.6888794 * jax.random.uniform(streams_of[8], (GROUPS, COLS), jnp.float32) ** shard_levels(streams_of[8], (GROUPS, COLS), ((0, 8),), -0.2, 0.2)), 0.1, 4.0)
    return dict(layer_inputs=layer_inputs, key_cotangent=key_cotangent, key_weights=key_weights, outer_momentum=outer_momentum, state_codes=state_codes, first_row_max=first_row_max, first_col_max=first_col_max, second_row_max=second_row_max, second_col_max=second_col_max)


beta_one = 0.9
beta_two = 0.95
bias_one = 1.0 - 0.9 ** 10
bias_two = 1.0 - 0.95 ** 10
adam_eps = 1e-08
inner_rate = 0.01
weight_decay = 0.1
outer_rate = 0.7
outer_beta = 0.9
stat_eps = 1e-06

def adam_moments(gradient, packed_codes, first_rows, first_cols, second_rows, second_cols):
    first_code = (packed_codes // 16).astype(jnp.float32)
    second_code = (packed_codes % 16).astype(jnp.float32)
    first_old = jnp.minimum(first_rows[:, None], first_cols[None, :]) * (first_code - 7.5) / 7.5
    second_old = jnp.minimum(second_rows[:, None], second_cols[None, :]) * ((second_code + 1.0) / 16.0) ** 2
    first_new = beta_one * first_old + (1.0 - beta_one) * gradient
    second_new = beta_two * second_old + (1.0 - beta_two) * gradient * gradient
    return (first_new, second_new)

def pseudo_step(first_new, second_new, weights_float):
    update = first_new / bias_one / (jnp.sqrt(second_new / bias_two) + adam_eps)
    return inner_rate * (update + weight_decay * weights_float)

def reference(layer_inputs, key_cotangent, key_weights, outer_momentum, state_codes, first_row_max, first_col_max, second_row_max, second_col_max):
    weights_float = key_weights.astype(jnp.float32)

    def group_step(running, inputs):
        tokens, cotangent, packed_codes, first_rows, first_cols, second_rows, second_cols = inputs
        token_blocks = tokens.reshape(N_FSDP, TOK_DEV, ROWS)
        grad_blocks = cotangent.reshape(N_FSDP, TOK_DEV, COLS)

        def add_term(accum, pair):
            partial_term = lax.dot_general(pair[0], pair[1], (((0,), (0,)), ((), ())), preferred_element_type=jnp.float32)
            rounded = lax.optimization_barrier(partial_term.astype(jnp.bfloat16))
            return (accum + rounded.astype(jnp.float32), None)
        gradient, unused = lax.scan(add_term, jnp.zeros((ROWS, COLS), jnp.float32), (token_blocks, grad_blocks))
        first_new, second_new = adam_moments(gradient, packed_codes, first_rows, first_cols, second_rows, second_cols)
        pseudo = pseudo_step(first_new, second_new, weights_float)
        first_rmax = lax.optimization_barrier(jnp.max(jnp.abs(first_new), axis=1)) + stat_eps
        first_cmax = lax.optimization_barrier(jnp.max(jnp.abs(first_new), axis=0)) + stat_eps
        second_rmax = lax.optimization_barrier(jnp.max(second_new, axis=1)) + stat_eps
        second_cmax = lax.optimization_barrier(jnp.max(second_new, axis=0)) + stat_eps
        first_state = (first_new / jnp.minimum(first_rmax[:, None], first_cmax[None, :])).astype(jnp.bfloat16)
        second_state = (second_new / jnp.minimum(second_rmax[:, None], second_cmax[None, :])).astype(jnp.bfloat16)
        return (running + pseudo, (first_state, second_state, first_rmax, first_cmax, second_rmax, second_cmax))
    running, results = lax.scan(group_step, jnp.zeros((ROWS, COLS), jnp.float32), (layer_inputs, key_cotangent, state_codes, first_row_max, first_col_max, second_row_max, second_col_max))
    averaged = running / N_GRP
    new_momentum = outer_beta * outer_momentum + averaged
    new_weights = weights_float - outer_rate * (averaged + outer_beta * new_momentum)
    weights_half = new_weights.astype(jnp.bfloat16)

    def project(tokens):
        return jnp.dot(tokens, weights_half, preferred_element_type=jnp.float32).astype(jnp.bfloat16)
    next_keys = lax.map(project, layer_inputs)
    first_state, second_state, first_rmax, first_cmax, second_rmax, second_cmax = results
    return (new_weights, new_momentum, first_state, second_state, first_rmax, first_cmax, second_rmax, second_cmax, next_keys)
```

```python
import functools
import jax
import jax.numpy as jnp
from jax import lax
from jax.experimental import pallas as pl
from jax.experimental.pallas import tpu as pltpu
from jax.sharding import PartitionSpec as P

MESH = pl.DeviceIdType.MESH
f32, bf16 = jnp.float32, jnp.bfloat16
beta_one = 0.9
beta_two = 0.95
bias_one = 1.0 - 0.9**10
bias_two = 1.0 - 0.95**10
adam_eps = 1e-08
inner_rate = 0.01
weight_decay = 0.1
outer_rate = 0.7
outer_beta = 0.9
stat_eps = 1e-06
TILE = 16


def to_column(row):
    return jnp.broadcast_to(row, (128, row.shape[1])).T[:, :1]


def to_row(column):
    return jnp.broadcast_to(column, (column.shape[0], 128)).T[:1, :]


def kernel(
    n, G, S, R, PR, NP,
    x_hbm, c_hbm, w_hbm, m_hbm, q_hbm, frm, fcm, srm, scm,
    o_w, o_m, o_fs, o_ss, o_frm, o_fcm, o_srm, o_scm, o_k,
    x, ct, w, m, q, tb, rb, pb, rp, av, wf, fn, sn, acc, fcol, scol, frn, srn, ca, cb, cmb,
    ld, ts, tr, ps, pr, as_, ar, gs, gr, hs, hr, cs, cr,
):
    g = lax.axis_index("grp")
    z = lax.axis_index("fsdp")
    rows = S * R
    C = w.shape[1]
    half = R // 2
    h = lax.rem(g, 2)
    mate = g + 1 - 2 * h

    loads = [
        pltpu.make_async_copy(src, dst, ld.at[i])
        for i, (src, dst) in enumerate(
            ((c_hbm, ct), (x_hbm, x), (q_hbm, q), (w_hbm, w), (m_hbm, m))
        )
    ]
    for load in loads:
        load.start()

    barrier = pltpu.get_barrier_semaphore()
    for d in range(1, G):
        pl.semaphore_signal(
            barrier, inc=1, device_id=(lax.rem(g + d, G), z), device_id_type=MESH
        )
    for d in range(1, n):
        pl.semaphore_signal(
            barrier, inc=1, device_id=(g, lax.rem(z + d, n)), device_id_type=MESH
        )

    for s in range(S):
        block = pl.ds(s * R, R)
        fcol[block, :] = to_column(frm[:, block])
        scol[block, :] = to_column(srm[:, block])
    ca[...] = jnp.zeros_like(ca)
    cb[...] = jnp.zeros_like(cb)

    pl.semaphore_wait(barrier, G - 1 + n - 1)
    loads[0].wait()
    loads[1].wait()

    def term(c, s):
        columns = pl.ds(pl.multiple_of(c * rows + s * R, 128), R)
        return lax.dot_general(
            x[:, columns], ct[...], (((0,), (0,)), ((), ())), preferred_element_type=f32
        )

    def move(s, c, slot, to):
        return pltpu.make_async_remote_copy(
            src_ref=tb.at[s, c], dst_ref=rb.at[s, slot], send_sem=ts.at[s, c],
            recv_sem=tr.at[s, slot], device_id=(g, to), device_id_type=MESH,
        )

    other_z = lax.rem(z + 1, n)

    def stream(s):
        def step(k, carry):
            right = n - 1 - k
            left = k

            @pl.when(right > z)
            def _():
                @pl.when(z == 0)
                def _():
                    tb[s, right] = term(right, s).astype(bf16)

                @pl.when(z > 0)
                def _():
                    own = term(right, s)
                    move(s, right, right, other_z).wait_recv()
                    tb[s, right] = (own + rb[s, right].astype(f32)).astype(bf16)

                move(s, right, right, z + 1).start()

            @pl.when(left < z)
            def _():
                @pl.when(z == n - 1)
                def _():
                    tb[s, left] = term(left, s).astype(bf16)

                @pl.when(z < n - 1)
                def _():
                    own = term(left, s)
                    move(s, left, left, other_z).wait_recv()
                    tb[s, left] = (own + rb[s, left].astype(f32)).astype(bf16)

                move(s, left, jnp.where(left == z - 1, n, left), z - 1).start()

            return carry

        lax.fori_loop(0, n - 1, step, 0)

    def piece(s, p, to):
        return pltpu.make_async_remote_copy(
            src_ref=pb.at[s, p], dst_ref=rp.at[s, g], send_sem=ps.at[s, p],
            recv_sem=pr.at[s, g], device_id=(to, z), device_id_type=MESH,
        )

    def piece_from(s, p):
        return pltpu.make_async_remote_copy(
            src_ref=pb.at[s, 0], dst_ref=rp.at[s, p], send_sem=ps.at[s, 0],
            recv_sem=pr.at[s, p], device_id=(mate, z), device_id_type=MESH,
        )

    def inner(s):
        acc[pl.ds(0, R), :] = term(z, s)

        @pl.when(z > 0)
        def _():
            move(s, z, z, other_z).wait_recv()
            acc[pl.ds(0, R), :] += rb[s, z].astype(f32)

        @pl.when(z < n - 1)
        def _():
            move(s, z, n, other_z).wait_recv()
            acc[pl.ds(0, R), :] += rb[s, n].astype(f32)

        def tile(i, carry):
            at = pl.multiple_of(i * TILE, TILE)
            place = pl.ds(pl.multiple_of(s * R + i * TILE, TILE), TILE)
            gradient = acc[pl.ds(at, TILE), :]
            codes = q[place, :]
            first_code = (codes >> 4).astype(f32)
            second_code = (codes & 15).astype(f32)
            first_old = jnp.minimum(fcol[place, :], fcm[...]) * ((first_code - 7.5) / 7.5)
            level = (second_code + 1.0) * (1.0 / 16.0)
            second_old = jnp.minimum(scol[place, :], scm[...]) * (level * level)
            first_new = beta_one * first_old + (1.0 - beta_one) * gradient
            second_new = beta_two * second_old + (1.0 - beta_two) * gradient * gradient
            fn[place, :] = first_new
            sn[place, :] = second_new
            update = (first_new / bias_one) / (jnp.sqrt(second_new / bias_two) + adam_eps)
            pseudo = inner_rate * (update + weight_decay * w[place, :].astype(f32))
            pb[s, i // (PR // TILE), pl.ds(lax.rem(i, PR // TILE) * TILE, TILE), :] = pseudo.astype(bf16)
            size = jnp.abs(first_new)
            ca[...] = jnp.maximum(ca[...], size)
            cb[...] = jnp.maximum(cb[...], second_new)
            frn[place, :] = jnp.max(size, axis=1, keepdims=True) + stat_eps
            srn[place, :] = jnp.max(second_new, axis=1, keepdims=True) + stat_eps
            return carry

        lax.fori_loop(0, R // TILE, tile, 0)

        def send(d, carry):
            p = lax.rem(g + d, G)

            @pl.when(p < NP)
            def _():
                piece(s, p, p).start()

            return carry

        lax.fori_loop(1, G, send, 0)

    def share(s, p, to):
        own = pl.ds(pl.multiple_of(p * PR, PR), PR)
        return pltpu.make_async_remote_copy(
            src_ref=av.at[s, own], dst_ref=av.at[s, own], send_sem=as_.at[s, to],
            recv_sem=ar.at[s, p], device_id=(to, z), device_id_type=MESH,
        )

    def reduce(s):
        @pl.when(g < NP)
        def _():
            acc[pl.ds(0, PR), :] = pb[s, g].astype(f32)

            def add(d, carry):
                p = lax.rem(g + d, G)
                piece_from(s, p).wait_recv()
                acc[pl.ds(0, PR), :] += rp[s, p].astype(f32)
                return carry

            lax.fori_loop(1, G, add, 0)
            av[s, pl.ds(pl.multiple_of(g * PR, PR), PR), :] = (
                acc[pl.ds(0, PR), :] * (1.0 / G)
            ).astype(bf16)

            def send(d, carry):
                share(s, g, lax.rem(g + d, G)).start()
                return carry

            lax.fori_loop(1, G, send, 0)

    def relay(s, c, way, to):
        part = pl.ds(pl.multiple_of(s * R + h * half, half), half)
        return pltpu.make_async_remote_copy(
            src_ref=wf.at[c, part], dst_ref=wf.at[c, part], send_sem=gs.at[way, s, c],
            recv_sem=gr.at[s, c], device_id=(g, to), device_id_type=MESH,
        )

    def hand(s, c):
        part = pl.ds(pl.multiple_of(s * R + h * half, half), half)
        return pltpu.make_async_remote_copy(
            src_ref=wf.at[c, part], dst_ref=wf.at[c, part], send_sem=hs.at[s, c],
            recv_sem=hr.at[s, c], device_id=(mate, z), device_id_type=MESH,
        )

    def hand_from(s, c):
        part = pl.ds(pl.multiple_of(s * R + (1 - h) * half, half), half)
        return pltpu.make_async_remote_copy(
            src_ref=wf.at[c, part], dst_ref=wf.at[c, part], send_sem=hs.at[s, c],
            recv_sem=hr.at[s, c], device_id=(mate, z), device_id_type=MESH,
        )

    def outer(s):
        def wait(p, carry):
            @pl.when(p != g)
            def _():
                share(s, p, mate).wait_recv()

            return carry

        lax.fori_loop(0, NP, wait, 0)

        def tile(i, carry):
            place = pl.ds(pl.multiple_of(s * R + i * TILE, TILE), TILE)
            averaged = av[s, pl.ds(pl.multiple_of(i * TILE, TILE), TILE), :].astype(f32)
            momentum = outer_beta * m[place, :] + averaged
            fresh = w[place, :].astype(f32) - outer_rate * (averaged + outer_beta * momentum)
            o_m[place, :] = momentum
            o_w[place, :] = fresh
            wf[z, place, :] = fresh.astype(bf16)
            return carry

        lax.fori_loop(0, R // TILE, tile, 0)

        @pl.when(z < n - 1)
        def _():
            relay(s, z, 0, z + 1).start()

        @pl.when(z > 0)
        def _():
            relay(s, z, 1, z - 1).start()

    def hop(s, j):
        @pl.when(z - j >= 0)
        def _():
            c = z - j
            relay(s, c, 0, other_z).wait_recv()

            @pl.when(z < n - 1)
            def _():
                relay(s, c, 0, z + 1).start()

            hand(s, c).start()

        @pl.when(z + j < n)
        def _():
            c = z + j
            relay(s, c, 1, other_z).wait_recv()

            @pl.when(z > 0)
            def _():
                relay(s, c, 1, z - 1).start()

            hand(s, c).start()

    def hops(u):
        for j in range(1, n):
            if (u - 3 - j) % 2 == 0 and 0 <= (u - 3 - j) // 2 < S:
                hop((u - 3 - j) // 2, j)

    @pl.when((z == 0) | (z == n - 1))
    def _():
        def every(s, carry):
            stream(s)
            return carry

        lax.fori_loop(0, S, every, 0)

    for load in loads[2:]:
        load.wait()

    def column_max(slot, to):
        return pltpu.make_async_remote_copy(
            src_ref=cmb.at[z], dst_ref=cmb.at[z], send_sem=cs.at[slot],
            recv_sem=cr.at[z], device_id=(g, to), device_id_type=MESH,
        )

    def column_max_from(c):
        return pltpu.make_async_remote_copy(
            src_ref=cmb.at[c], dst_ref=cmb.at[c], send_sem=cs.at[0],
            recv_sem=cr.at[c], device_id=(g, other_z), device_id_type=MESH,
        )

    for s in range(S + 1):
        if s < S:
            @pl.when((z > 0) & (z < n - 1))
            def _():
                stream(s)
        hops(2 * s)
        if s >= 1:
            reduce(s - 1)
        if s < S:
            inner(s)
        if s == S - 1:
            cmb[z, pl.ds(0, 1), :] = jnp.max(ca[...], axis=0, keepdims=True)
            cmb[z, pl.ds(1, 1), :] = jnp.max(cb[...], axis=0, keepdims=True)
            for d in range(1, n):
                column_max(d, lax.rem(z + d, n)).start()
        if s >= 1:
            outer(s - 1)
        hops(2 * s + 1)

    for d in range(1, n):
        column_max_from(lax.rem(z + d, n)).wait_recv()
    scales = jnp.max(cmb[...], axis=0) + stat_eps
    o_fcm[...] = scales[0:1]
    o_scm[...] = scales[1:2]

    def states(s):
        def tile(i, carry):
            place = pl.ds(pl.multiple_of(s * R + i * TILE, TILE), TILE)
            o_fs[place, :] = (fn[place, :] / jnp.minimum(frn[place, :], o_fcm[...])).astype(bf16)
            o_ss[place, :] = (sn[place, :] / jnp.minimum(srn[place, :], o_scm[...])).astype(bf16)
            return carry

        lax.fori_loop(0, R // TILE, tile, 0)
        block = pl.ds(s * R, R)
        o_frm[:, block] = to_row(frn[block, :])
        o_srm[:, block] = to_row(srn[block, :])

    for s in range(S):
        states(s)

    def product(c):
        columns = pl.ds(pl.multiple_of(c * rows, 128), rows)
        return jnp.dot(x[:, columns], wf[c], preferred_element_type=f32)

    acc[...] = product(z)
    for u in range(2 * S + 2, 2 * S + 2 + n - 1):
        hops(u)

    def gather(j, carry):
        for c in (z - j, z + j):
            @pl.when((c >= 0) & (c < n))
            def _():
                for s in range(S):
                    hand_from(s, c).wait_recv()
                acc[...] += product(c)
        return carry

    lax.fori_loop(1, n, gather, 0)
    o_k[...] = acc[...].astype(bf16)

    for s in range(S):
        def sent(c, carry):
            @pl.when(c != z)
            def _():
                move(s, c, c, other_z).wait_send()
                hand(s, c).wait_send()

            @pl.when((c <= z) & (z < n - 1))
            def _():
                relay(s, c, 0, other_z).wait_send()

            @pl.when((c >= z) & (z > 0))
            def _():
                relay(s, c, 1, other_z).wait_send()

            return carry

        lax.fori_loop(0, n, sent, 0)

        def plane(p, carry):
            @pl.when(p != g)
            def _():
                @pl.when(p < NP)
                def _():
                    piece(s, p, mate).wait_send()

                @pl.when(g < NP)
                def _():
                    share(s, g, p).wait_send()

            return carry

        lax.fori_loop(0, G, plane, 0)
    for d in range(1, n):
        column_max(d, other_z).wait_send()


def local(x, ct, w, m, q, frm, fcm, srm, scm):
    n, G = lax.axis_size("fsdp"), lax.axis_size("grp")
    rows, C = w.shape
    T, K = x.shape[1:]
    R = min(128, rows)
    S = rows // R
    PR = max(TILE, R // G)
    NP = R // PR
    hbm = pl.BlockSpec(memory_space=pl.ANY)
    vmem = pl.BlockSpec(memory_space=pltpu.VMEM)
    dma = pltpu.SemaphoreType.DMA
    shape = jax.ShapeDtypeStruct
    outs = pl.pallas_call(
        functools.partial(kernel, n, G, S, R, PR, NP),
        out_shape=(
            shape((rows, C), f32), shape((rows, C), f32),
            shape((rows, C), bf16), shape((rows, C), bf16),
            shape((1, rows), f32), shape((1, C), f32),
            shape((1, rows), f32), shape((1, C), f32),
            shape((T, C), bf16),
        ),
        in_specs=[hbm] * 5 + [vmem] * 4,
        out_specs=(vmem,) * 9,
        scratch_shapes=[
            pltpu.VMEM((T, K), bf16), pltpu.VMEM((T, C), bf16), pltpu.VMEM((rows, C), bf16),
            pltpu.VMEM((rows, C), f32), pltpu.VMEM((rows, C), jnp.int32),
            pltpu.VMEM((S, n, R, C), bf16), pltpu.VMEM((S, n + 1, R, C), bf16),
            pltpu.VMEM((S, NP, PR, C), bf16), pltpu.VMEM((S, G, PR, C), bf16),
            pltpu.VMEM((S, R, C), bf16), pltpu.VMEM((n, rows, C), bf16),
            pltpu.VMEM((rows, C), f32), pltpu.VMEM((rows, C), f32), pltpu.VMEM((T, C), f32),
            pltpu.VMEM((rows, 1), f32), pltpu.VMEM((rows, 1), f32),
            pltpu.VMEM((rows, 1), f32), pltpu.VMEM((rows, 1), f32),
            pltpu.VMEM((TILE, C), f32), pltpu.VMEM((TILE, C), f32), pltpu.VMEM((n, 2, C), f32),
            dma((5,)), dma((S, n)), dma((S, n + 1)), dma((S, NP)), dma((S, G)),
            dma((S, G)), dma((S, NP)), dma((2, S, n)), dma((S, n)), dma((S, n)), dma((S, n)),
            dma((n,)), dma((n,)),
        ],
        compiler_params=pltpu.CompilerParams(
            collective_id=0, has_side_effects=True, vmem_limit_bytes=60 * 1024 * 1024
        ),
    )(x[0], ct[0], w, m, q[0], frm, fcm, srm, scm)
    new_w, new_m, fs, ss, nfr, nfc, nsr, nsc, keys = outs
    return new_w, new_m, fs[None], ss[None], nfr, nfc, nsr, nsc, keys[None]


def solution(mesh):
    return jax.shard_map(
        local,
        mesh=mesh,
        in_specs=(
            P("grp", "fsdp", None), P("grp", "fsdp", None), P("fsdp", None), P("fsdp", None),
            P("grp", "fsdp", None), P("grp", "fsdp"), P("grp", None), P("grp", "fsdp"),
            P("grp", None),
        ),
        out_specs=(
            P("fsdp", None), P("fsdp", None), P("grp", "fsdp", None), P("grp", "fsdp", None),
            P("grp", "fsdp"), P("grp", None), P("grp", "fsdp"), P("grp", None),
            P("grp", "fsdp", None),
        ),
        check_vma=False,
    )
```

```python
import functools
import jax
import jax.numpy as jnp
from jax import lax
from jax.experimental import pallas as pl
from jax.experimental.pallas import tpu as pltpu
from jax.sharding import PartitionSpec as P

MESH = pl.DeviceIdType.MESH
f32, bf16 = jnp.float32, jnp.bfloat16
beta_one = 0.9
beta_two = 0.95
bias_one = 1.0 - 0.9**10
bias_two = 1.0 - 0.95**10
adam_eps = 1e-08
inner_rate = 0.01
weight_decay = 0.1
outer_rate = 0.7
outer_beta = 0.9
stat_eps = 1e-06
TILE = 16


def to_column(row):
    return jnp.broadcast_to(row, (128, row.shape[1])).T[:, :1]


def to_row(column):
    return jnp.broadcast_to(column, (column.shape[0], 128)).T[:1, :]


def kernel(
    n, G, S, R, PR, NP,
    x_hbm, c_hbm, w_hbm, m_hbm, q_hbm, frm, fcm, srm, scm,
    o_a, o_fs, o_ss, o_frm, o_fcm, o_srm, o_scm, o_k,
    x, ct, w, m, q, tb, rb, pb, rp, av, wf, fn, sn, acc, fcol, scol, frn, srn, ca, cb, cmb,
    ld, ts, tr, ps, pr, as_, ar, gs, gr, hs, hr, cs, cr,
):
    g = lax.axis_index("grp")
    z = lax.axis_index("fsdp")
    rows = S * R
    C = w.shape[1]
    half = R // 2
    h = lax.rem(g, 2)
    mate = g + 1 - 2 * h

    loads = [
        pltpu.make_async_copy(src, dst, ld.at[i])
        for i, (src, dst) in enumerate(
            ((c_hbm, ct), (x_hbm, x), (q_hbm, q), (w_hbm, w), (m_hbm, m))
        )
    ]
    for load in loads:
        load.start()

    barrier = pltpu.get_barrier_semaphore()
    for d in range(1, G):
        pl.semaphore_signal(
            barrier, inc=1, device_id=(lax.rem(g + d, G), z), device_id_type=MESH
        )
    for d in range(1, n):
        pl.semaphore_signal(
            barrier, inc=1, device_id=(g, lax.rem(z + d, n)), device_id_type=MESH
        )

    for s in range(S):
        block = pl.ds(s * R, R)
        fcol[block, :] = to_column(frm[:, block])
        scol[block, :] = to_column(srm[:, block])
    ca[...] = jnp.zeros_like(ca)
    cb[...] = jnp.zeros_like(cb)

    pl.semaphore_wait(barrier, G - 1 + n - 1)
    loads[0].wait()
    loads[1].wait()

    def term(c, s):
        columns = pl.ds(pl.multiple_of(c * rows + s * R, 128), R)
        return lax.dot_general(
            x[:, columns], ct[...], (((0,), (0,)), ((), ())), preferred_element_type=f32
        )

    def move(s, c, slot, to):
        return pltpu.make_async_remote_copy(
            src_ref=tb.at[s, c], dst_ref=rb.at[s, slot], send_sem=ts.at[s, c],
            recv_sem=tr.at[s, slot], device_id=(g, to), device_id_type=MESH,
        )

    other_z = lax.rem(z + 1, n)

    def stream(s):
        def step(k, carry):
            right = n - 1 - k
            left = k

            @pl.when(right > z)
            def _():
                @pl.when(z == 0)
                def _():
                    tb[s, right] = term(right, s).astype(bf16)

                @pl.when(z > 0)
                def _():
                    own = term(right, s)
                    move(s, right, right, other_z).wait_recv()
                    tb[s, right] = (own + rb[s, right].astype(f32)).astype(bf16)

                move(s, right, right, z + 1).start()

            @pl.when(left < z)
            def _():
                @pl.when(z == n - 1)
                def _():
                    tb[s, left] = term(left, s).astype(bf16)

                @pl.when(z < n - 1)
                def _():
                    own = term(left, s)
                    move(s, left, left, other_z).wait_recv()
                    tb[s, left] = (own + rb[s, left].astype(f32)).astype(bf16)

                move(s, left, jnp.where(left == z - 1, n, left), z - 1).start()

            return carry

        lax.fori_loop(0, n - 1, step, 0)

    def piece(s, p, to):
        return pltpu.make_async_remote_copy(
            src_ref=pb.at[s, p], dst_ref=rp.at[s, g], send_sem=ps.at[s, p],
            recv_sem=pr.at[s, g], device_id=(to, z), device_id_type=MESH,
        )

    def piece_from(s, p):
        return pltpu.make_async_remote_copy(
            src_ref=pb.at[s, 0], dst_ref=rp.at[s, p], send_sem=ps.at[s, 0],
            recv_sem=pr.at[s, p], device_id=(mate, z), device_id_type=MESH,
        )

    def inner(s):
        acc[pl.ds(0, R), :] = term(z, s)

        @pl.when(z > 0)
        def _():
            move(s, z, z, other_z).wait_recv()
            acc[pl.ds(0, R), :] += rb[s, z].astype(f32)

        @pl.when(z < n - 1)
        def _():
            move(s, z, n, other_z).wait_recv()
            acc[pl.ds(0, R), :] += rb[s, n].astype(f32)

        def tile(i, carry):
            at = pl.multiple_of(i * TILE, TILE)
            place = pl.ds(pl.multiple_of(s * R + i * TILE, TILE), TILE)
            gradient = acc[pl.ds(at, TILE), :]
            codes = q[place, :]
            first_code = (codes >> 4).astype(f32)
            second_code = (codes & 15).astype(f32)
            first_old = jnp.minimum(fcol[place, :], fcm[...]) * ((first_code - 7.5) / 7.5)
            level = (second_code + 1.0) * (1.0 / 16.0)
            second_old = jnp.minimum(scol[place, :], scm[...]) * (level * level)
            first_new = beta_one * first_old + (1.0 - beta_one) * gradient
            second_new = beta_two * second_old + (1.0 - beta_two) * gradient * gradient
            fn[place, :] = first_new
            sn[place, :] = second_new
            update = (first_new / bias_one) / (jnp.sqrt(second_new / bias_two) + adam_eps)
            pseudo = inner_rate * (update + weight_decay * w[place, :].astype(f32))
            pb[s, i // (PR // TILE), pl.ds(lax.rem(i, PR // TILE) * TILE, TILE), :] = pseudo.astype(bf16)
            size = jnp.abs(first_new)
            ca[...] = jnp.maximum(ca[...], size)
            cb[...] = jnp.maximum(cb[...], second_new)
            frn[place, :] = jnp.max(size, axis=1, keepdims=True) + stat_eps
            srn[place, :] = jnp.max(second_new, axis=1, keepdims=True) + stat_eps
            return carry

        lax.fori_loop(0, R // TILE, tile, 0)

        def send(d, carry):
            p = lax.rem(g + d, G)

            @pl.when(p < NP)
            def _():
                piece(s, p, p).start()

            return carry

        lax.fori_loop(1, G, send, 0)

    def share(s, p, to):
        own = pl.ds(pl.multiple_of(p * PR, PR), PR)
        return pltpu.make_async_remote_copy(
            src_ref=av.at[s, own], dst_ref=av.at[s, own], send_sem=as_.at[s, to],
            recv_sem=ar.at[s, p], device_id=(to, z), device_id_type=MESH,
        )

    def reduce(s):
        @pl.when(g < NP)
        def _():
            acc[pl.ds(0, PR), :] = pb[s, g].astype(f32)

            def add(d, carry):
                p = lax.rem(g + d, G)
                piece_from(s, p).wait_recv()
                acc[pl.ds(0, PR), :] += rp[s, p].astype(f32)
                return carry

            lax.fori_loop(1, G, add, 0)
            av[s, pl.ds(pl.multiple_of(g * PR, PR), PR), :] = (
                acc[pl.ds(0, PR), :] * (1.0 / G)
            ).astype(bf16)

            def send(d, carry):
                share(s, g, lax.rem(g + d, G)).start()
                return carry

            lax.fori_loop(1, G, send, 0)

    def relay(s, c, way, to):
        part = pl.ds(pl.multiple_of(s * R + h * half, half), half)
        return pltpu.make_async_remote_copy(
            src_ref=wf.at[c, part], dst_ref=wf.at[c, part], send_sem=gs.at[way, s, c],
            recv_sem=gr.at[s, c], device_id=(g, to), device_id_type=MESH,
        )

    def hand(s, c):
        part = pl.ds(pl.multiple_of(s * R + h * half, half), half)
        return pltpu.make_async_remote_copy(
            src_ref=wf.at[c, part], dst_ref=wf.at[c, part], send_sem=hs.at[s, c],
            recv_sem=hr.at[s, c], device_id=(mate, z), device_id_type=MESH,
        )

    def hand_from(s, c):
        part = pl.ds(pl.multiple_of(s * R + (1 - h) * half, half), half)
        return pltpu.make_async_remote_copy(
            src_ref=wf.at[c, part], dst_ref=wf.at[c, part], send_sem=hs.at[s, c],
            recv_sem=hr.at[s, c], device_id=(mate, z), device_id_type=MESH,
        )

    def outer(s):
        def wait(p, carry):
            @pl.when(p != g)
            def _():
                share(s, p, mate).wait_recv()

            return carry

        lax.fori_loop(0, NP, wait, 0)

        def tile(i, carry):
            place = pl.ds(pl.multiple_of(s * R + i * TILE, TILE), TILE)
            sent = av[s, pl.ds(pl.multiple_of(i * TILE, TILE), TILE), :]
            o_a[place, :] = sent
            averaged = sent.astype(f32)
            momentum = outer_beta * m[place, :] + averaged
            fresh = w[place, :].astype(f32) - outer_rate * (averaged + outer_beta * momentum)
            wf[z, place, :] = fresh.astype(bf16)
            return carry

        lax.fori_loop(0, R // TILE, tile, 0)

        @pl.when(z < n - 1)
        def _():
            relay(s, z, 0, z + 1).start()

        @pl.when(z > 0)
        def _():
            relay(s, z, 1, z - 1).start()

    def hop(s, j):
        @pl.when(z - j >= 0)
        def _():
            c = z - j
            relay(s, c, 0, other_z).wait_recv()

            @pl.when(z < n - 1)
            def _():
                relay(s, c, 0, z + 1).start()

            hand(s, c).start()

        @pl.when(z + j < n)
        def _():
            c = z + j
            relay(s, c, 1, other_z).wait_recv()

            @pl.when(z > 0)
            def _():
                relay(s, c, 1, z - 1).start()

            hand(s, c).start()

    def hops(u):
        for j in range(1, n):
            if (u - 3 - j) % 2 == 0 and 0 <= (u - 3 - j) // 2 < S:
                hop((u - 3 - j) // 2, j)

    @pl.when((z == 0) | (z == n - 1))
    def _():
        def every(s, carry):
            stream(s)
            return carry

        lax.fori_loop(0, S, every, 0)

    for load in loads[2:]:
        load.wait()

    def column_max(slot, to):
        return pltpu.make_async_remote_copy(
            src_ref=cmb.at[z], dst_ref=cmb.at[z], send_sem=cs.at[slot],
            recv_sem=cr.at[z], device_id=(g, to), device_id_type=MESH,
        )

    def column_max_from(c):
        return pltpu.make_async_remote_copy(
            src_ref=cmb.at[c], dst_ref=cmb.at[c], send_sem=cs.at[0],
            recv_sem=cr.at[c], device_id=(g, other_z), device_id_type=MESH,
        )

    for s in range(S + 1):
        if s < S:
            @pl.when((z > 0) & (z < n - 1))
            def _():
                stream(s)
        hops(2 * s)
        if s >= 1:
            reduce(s - 1)
        if s < S:
            inner(s)
        if s == S - 1:
            cmb[z, pl.ds(0, 1), :] = jnp.max(ca[...], axis=0, keepdims=True)
            cmb[z, pl.ds(1, 1), :] = jnp.max(cb[...], axis=0, keepdims=True)
            for d in range(1, n):
                column_max(d, lax.rem(z + d, n)).start()
        if s >= 1:
            outer(s - 1)
        hops(2 * s + 1)

    for d in range(1, n):
        column_max_from(lax.rem(z + d, n)).wait_recv()
    scales = jnp.max(cmb[...], axis=0) + stat_eps
    o_fcm[...] = scales[0:1]
    o_scm[...] = scales[1:2]

    def states(s):
        def tile(i, carry):
            place = pl.ds(pl.multiple_of(s * R + i * TILE, TILE), TILE)
            o_fs[place, :] = (fn[place, :] / jnp.minimum(frn[place, :], o_fcm[...])).astype(bf16)
            o_ss[place, :] = (sn[place, :] / jnp.minimum(srn[place, :], o_scm[...])).astype(bf16)
            return carry

        lax.fori_loop(0, R // TILE, tile, 0)
        block = pl.ds(s * R, R)
        o_frm[:, block] = to_row(frn[block, :])
        o_srm[:, block] = to_row(srn[block, :])

    for s in range(S):
        states(s)

    def product(c):
        columns = pl.ds(pl.multiple_of(c * rows, 128), rows)
        return jnp.dot(x[:, columns], wf[c], preferred_element_type=f32)

    acc[...] = product(z)
    for u in range(2 * S + 2, 2 * S + 2 + n - 1):
        hops(u)

    def gather(j, carry):
        for c in (z - j, z + j):
            @pl.when((c >= 0) & (c < n))
            def _():
                for s in range(S):
                    hand_from(s, c).wait_recv()
                acc[...] += product(c)
        return carry

    lax.fori_loop(1, n, gather, 0)
    o_k[...] = acc[...].astype(bf16)

    for s in range(S):
        def sent(c, carry):
            @pl.when(c != z)
            def _():
                move(s, c, c, other_z).wait_send()
                hand(s, c).wait_send()

            @pl.when((c <= z) & (z < n - 1))
            def _():
                relay(s, c, 0, other_z).wait_send()

            @pl.when((c >= z) & (z > 0))
            def _():
                relay(s, c, 1, other_z).wait_send()

            return carry

        lax.fori_loop(0, n, sent, 0)

        def plane(p, carry):
            @pl.when(p != g)
            def _():
                @pl.when(p < NP)
                def _():
                    piece(s, p, mate).wait_send()

                @pl.when(g < NP)
                def _():
                    share(s, g, p).wait_send()

            return carry

        lax.fori_loop(0, G, plane, 0)
    for d in range(1, n):
        column_max(d, other_z).wait_send()


def finish(avg, w, m, *refs):
    o_w, o_m = refs[7:9]
    averaged = avg[...].astype(f32)
    momentum = outer_beta * m[...] + averaged
    o_m[...] = momentum
    o_w[...] = w[...].astype(f32) - outer_rate * (averaged + outer_beta * momentum)
    for src, dst in zip(refs[:7], refs[9:]):
        dst[...] = src[...]


def local(x, ct, w, m, q, frm, fcm, srm, scm):
    n, G = lax.axis_size("fsdp"), lax.axis_size("grp")
    rows, C = w.shape
    T, K = x.shape[1:]
    R = min(128, rows)
    S = rows // R
    PR = max(TILE, R // G)
    NP = R // PR
    hbm = pl.BlockSpec(memory_space=pl.ANY)
    vmem = pl.BlockSpec(memory_space=pltpu.VMEM)
    dma = pltpu.SemaphoreType.DMA
    shape = jax.ShapeDtypeStruct
    outs = pl.pallas_call(
        functools.partial(kernel, n, G, S, R, PR, NP),
        out_shape=(
            shape((rows, C), bf16), shape((rows, C), bf16), shape((rows, C), bf16),
            shape((1, rows), f32), shape((1, C), f32),
            shape((1, rows), f32), shape((1, C), f32),
            shape((T, C), bf16),
        ),
        in_specs=[hbm] * 5 + [vmem] * 4,
        out_specs=(vmem,) * 8,
        scratch_shapes=[
            pltpu.VMEM((T, K), bf16), pltpu.VMEM((T, C), bf16), pltpu.VMEM((rows, C), bf16),
            pltpu.VMEM((rows, C), f32), pltpu.VMEM((rows, C), jnp.int32),
            pltpu.VMEM((S, n, R, C), bf16), pltpu.VMEM((S, n + 1, R, C), bf16),
            pltpu.VMEM((S, NP, PR, C), bf16), pltpu.VMEM((S, G, PR, C), bf16),
            pltpu.VMEM((S, R, C), bf16), pltpu.VMEM((n, rows, C), bf16),
            pltpu.VMEM((rows, C), f32), pltpu.VMEM((rows, C), f32), pltpu.VMEM((T, C), f32),
            pltpu.VMEM((rows, 1), f32), pltpu.VMEM((rows, 1), f32),
            pltpu.VMEM((rows, 1), f32), pltpu.VMEM((rows, 1), f32),
            pltpu.VMEM((TILE, C), f32), pltpu.VMEM((TILE, C), f32), pltpu.VMEM((n, 2, C), f32),
            dma((5,)), dma((S, n)), dma((S, n + 1)), dma((S, NP)), dma((S, G)),
            dma((S, G)), dma((S, NP)), dma((2, S, n)), dma((S, n)), dma((S, n)), dma((S, n)),
            dma((n,)), dma((n,)),
        ],
        compiler_params=pltpu.CompilerParams(
            collective_id=0, has_side_effects=True, vmem_limit_bytes=60 * 1024 * 1024
        ),
    )(x[0], ct[0], w, m, q[0], frm, fcm, srm, scm)
    avg, fs, ss, nfr, nfc, nsr, nsc, keys = outs
    steps = 4
    high = pl.BlockSpec((rows // steps, C), lambda i: (i, 0))
    tall = pl.BlockSpec((T // steps, C), lambda i: (i, 0))
    wide = pl.BlockSpec((1, rows), lambda i: (0, 0))
    flat = pl.BlockSpec((1, C), lambda i: (0, 0))
    blocks = (high, high, tall, wide, flat, wide, flat)
    new_w, new_m, fs, ss, keys, nfr, nfc, nsr, nsc = pl.pallas_call(
        finish,
        grid=(steps,),
        out_shape=(
            shape((rows, C), f32), shape((rows, C), f32),
            shape((rows, C), bf16), shape((rows, C), bf16), shape((T, C), bf16),
            shape((1, rows), f32), shape((1, C), f32),
            shape((1, rows), f32), shape((1, C), f32),
        ),
        in_specs=(high,) * 3 + blocks,
        out_specs=(high,) * 2 + blocks,
    )(avg, w, m, fs, ss, keys, nfr, nfc, nsr, nsc)
    return new_w, new_m, fs[None], ss[None], nfr, nfc, nsr, nsc, keys[None]


def solution(mesh):
    return jax.shard_map(
        local,
        mesh=mesh,
        in_specs=(
            P("grp", "fsdp", None), P("grp", "fsdp", None), P("fsdp", None), P("fsdp", None),
            P("grp", "fsdp", None), P("grp", "fsdp"), P("grp", None), P("grp", "fsdp"),
            P("grp", None),
        ),
        out_specs=(
            P("fsdp", None), P("fsdp", None), P("grp", "fsdp", None), P("grp", "fsdp", None),
            P("grp", "fsdp"), P("grp", None), P("grp", "fsdp"), P("grp", None),
            P("grp", "fsdp", None),
        ),
        check_vma=False,
    )
```
